32 devices in a mesh: groups: 2 (over x), patch: 16 (over z, y, core).
Axes of the slice: x: 2, y: 2, z: 4, core: 2. Of those that a mesh axis runs over, the one named last changes fastest.
Arguments:
- tokens: bfloat16 [16384, 1152], P(('groups', 'patch')), parts along dimension 0, may hold values from -6 to 6
- stale_kv: bfloat16 [16384, 1152], P(('groups', 'patch')), parts along dimension 0, may hold values from -40 to 40, as said below
- mod_table: float32 [6, 1152], replicated, may hold values from -2 to 3
- mod_mix: float32 [6, 1152], replicated, may hold values from -3 to 3
- timestep: int32 [2], P('groups'), parts along dimension 0, may hold values from 0 to 999
- frame_order: int32 [8], P('groups'), parts along dimension 0, may hold values from 0 to 3, each once
- spatial_qkv: bfloat16 [3, 1152, 576], replicated, may hold values from -0.1875 to 0.1875
- spatial_out: bfloat16 [576, 1152], replicated, may hold values from -0.25 to 0.25
- temporal_qkv: bfloat16 [3, 1152, 576], replicated, may hold values from -0.1875 to 0.1875
- temporal_out: bfloat16 [576, 1152], replicated, may hold values from -0.25 to 0.25
Outputs:
- block_out: float32 [16384, 1152], P(('groups', 'patch')), parts along dimension 0
The draws below stay inside these ranges and needn't reach their ends.
There are 2 independent parts, one for each index of `groups`. The reference program is written for one: setup_inputs(seed, part) draws one part's arguments, and reference() takes and returns one part's arrays. A program takes and returns all parts, laid end to end along the dimension named above; an argument that names none is the same for every part. Nothing has to cross between parts.
Inputs may be any that keep to these rules, and one draw needn't show every extreme that they name: `frame_order`: a permutation of the 4 time positions. `stale_kv`: previous step's keys and values.
All inputs are finite; a program needn't handle non-finite values.
Results may differ from the reference program's by a relative error of at most 0.013.
The reference program's roundings to bfloat16 on the way count: a program that leaves them out, or rounds other values in their place, can miss the bound.
Values may be sent and summed in bfloat16 or wider, within the bound.
A program may use at most 128 MiB of HBM per device.

```python
import math
import jax
import jax.numpy as jnp
from jax import lax

D = 1152
HEADS = 16
HEADS_WIN = 8
WIN = 576
PATCH_TOK = 512
FRAMES = 4
FRAME_TOK = 2048
TOKENS = 8192


def draw_stale_kv(key, part):
    width_win = HEADS_WIN * (D // HEADS)
    base = jnp.clip(jax.random.normal(jax.random.fold_in(key, 11), (TOKENS, 2 * width_win), jnp.float32), -5.0, 5.0)
    return base.astype(jnp.bfloat16)


def draw_mod_table(key, part):
    table = jnp.clip(0.5 * jax.random.normal(jax.random.fold_in(key, 21), (6, D), jnp.float32), -2.0, 2.0)
    return table


def levels(rng, shape, split, smallest, largest):
    loudness, own = 1.0, jax.random.fold_in(rng, 6)
    for axis_at, blocks in split:
        heights = jnp.exp(jax.random.uniform(jax.random.fold_in(own, axis_at), (blocks,), jnp.float32, smallest / len(split), largest / len(split)))
        loudness = loudness * jnp.repeat(heights, shape[axis_at] // blocks).reshape([-1 if axis == axis_at else 1 for axis in range(len(shape))])
    return loudness


def scatter_about(own_key, shape, width, limit, shards=(), kind=jnp.bfloat16):
    entries = jax.random.normal(own_key, shape, jnp.float32) * width
    if len(shards) > 0:
        entries = levels(own_key, shape, shards, -0.22, 0.18) * entries
    return jnp.clip(entries, min=-limit, max=limit).astype(kind)


def setup_inputs(seed: int = 0, part: int = 0) -> dict:
    key_list = jax.random.split(jax.random.key(seed), 11)
    part_keys = jax.random.split(jax.random.fold_in(key_list[10], part), 11)
    tokens = scatter_about(part_keys[0], (TOKENS, D), 1.0, 6.0, ((0, 16),))
    stale_kv = draw_stale_kv(jax.random.fold_in(jax.random.fold_in(key_list[10], part), 71), part)
    mod_table = draw_mod_table(jax.random.fold_in(key_list[10], 71), part)
    mod_mix = scatter_about(key_list[3], (6, D), 0.5, 3.0, (), jnp.float32)
    timestep = jax.random.randint(part_keys[4], (1,), 0, 1000).astype(jnp.int32)
    frame_order = jax.random.permutation(part_keys[5], FRAMES).astype(jnp.int32)
    spatial_qkv = scatter_about(key_list[6], (3, D, WIN), D ** -0.5, 0.1875)
    spatial_out = scatter_about(key_list[7], (WIN, D), WIN ** -0.5, 0.25)
    temporal_qkv = scatter_about(key_list[8], (3, D, WIN), D ** -0.5, 0.1875)
    temporal_out = scatter_about(key_list[9], (WIN, D), WIN ** -0.5, 0.25)
    return {"tokens": tokens, "stale_kv": stale_kv, "mod_table": mod_table, "mod_mix": mod_mix, "timestep": timestep, "frame_order": frame_order, "spatial_qkv": spatial_qkv, "spatial_out": spatial_out, "temporal_qkv": temporal_qkv, "temporal_out": temporal_out}


epsilon = 1e-06

def normalize(activations):
    row_mean = lax.optimization_barrier(jnp.mean(activations, axis=-1, keepdims=True))
    centered = activations - row_mean
    variance = lax.optimization_barrier(jnp.mean(centered * centered, axis=-1, keepdims=True))
    return centered * lax.rsqrt(variance + epsilon)

def sinusoid(position, feature_width):
    half_width = feature_width // 2
    frequencies = jnp.exp(-math.log(10000.0) * jnp.arange(half_width, dtype=jnp.float32) / half_width)
    angles = jnp.asarray(position).astype(jnp.float32)[..., None] * frequencies
    return jnp.concatenate([jnp.sin(angles), jnp.cos(angles)], axis=-1)

def softmax_rows(scores):
    row_top = lax.optimization_barrier(jnp.max(scores, axis=-1, keepdims=True))
    exp_scores = jnp.exp(scores - row_top)
    return (exp_scores / lax.optimization_barrier(jnp.sum(exp_scores, axis=-1, keepdims=True))).astype(jnp.bfloat16)

def project(inputs, weight):
    return jnp.dot(inputs, weight, preferred_element_type=jnp.float32)

def spatial_attend(queries, key_rows, value_rows):
    head_dim = D // HEADS
    query_heads = queries.reshape(-1, HEADS_WIN, head_dim).astype(jnp.float32)
    key_heads = key_rows.reshape(-1, HEADS_WIN, head_dim).astype(jnp.float32)
    value_heads = value_rows.reshape(-1, HEADS_WIN, head_dim).astype(jnp.float32)
    scores = jnp.einsum('qhe,khe->hqk', query_heads, key_heads) * head_dim ** (-0.5)
    weights = softmax_rows(scores)
    mixed_out = jnp.einsum('hqk,khe->qhe', weights.astype(jnp.float32), value_heads)
    return mixed_out.reshape(-1, HEADS_WIN * head_dim).astype(jnp.bfloat16)

def temporal_attend(queries, key_rows, value_rows):
    head_dim = D // HEADS
    frame_count = queries.shape[0]
    pixel_count = queries.shape[1]
    shape_heads = (frame_count, pixel_count, HEADS_WIN, head_dim)
    query_heads = queries.reshape(shape_heads).astype(jnp.float32)
    key_heads = key_rows.reshape(shape_heads).astype(jnp.float32)
    value_heads = value_rows.reshape(shape_heads).astype(jnp.float32)
    scores = jnp.einsum('fmhe,gmhe->mhfg', query_heads, key_heads) * head_dim ** (-0.5)
    weights = softmax_rows(scores)
    mixed_out = jnp.einsum('mhfg,gmhe->fmhe', weights.astype(jnp.float32), value_heads)
    return mixed_out.reshape(frame_count, pixel_count, HEADS_WIN * head_dim).astype(jnp.bfloat16)

def reference(tokens, stale_kv, mod_table, mod_mix, timestep, frame_order, spatial_qkv, spatial_out, temporal_qkv, temporal_out):
    width_win = HEADS_WIN * (D // HEADS)
    modulation = mod_table + mod_mix * sinusoid(timestep[0], D)[None, :]
    tokens_wide = tokens.astype(jnp.float32)
    spatial_in = (normalize(tokens_wide) * (1.0 + modulation[1]) + modulation[0]).astype(jnp.bfloat16)
    quartered = (FRAMES, 4, PATCH_TOK, width_win)
    fresh_q = project(spatial_in, spatial_qkv[0]).astype(jnp.bfloat16).reshape(quartered)
    fresh_k = project(spatial_in, spatial_qkv[1]).astype(jnp.bfloat16).reshape(quartered)
    fresh_v = project(spatial_in, spatial_qkv[2]).astype(jnp.bfloat16).reshape(quartered)
    stale_k = stale_kv[:, :width_win].reshape(quartered)
    stale_v = stale_kv[:, width_win:].reshape(quartered)

    def one_frame(inputs):
        frame_q, frame_k, frame_v, old_k, old_v = inputs
        results = []
        for quarter in range(4):
            key_rows = jnp.concatenate([frame_k[source] if source == quarter else old_k[source] for source in range(4)], axis=0)
            value_rows = jnp.concatenate([frame_v[source] if source == quarter else old_v[source] for source in range(4)], axis=0)
            results.append(spatial_attend(frame_q[quarter], key_rows, value_rows))
        return jnp.stack(results)
    spatial_mixed = lax.map(one_frame, (fresh_q, fresh_k, fresh_v, stale_k, stale_v)).reshape(TOKENS, width_win)
    after_spatial = tokens_wide + modulation[2] * project(spatial_mixed, spatial_out)
    positions = sinusoid(frame_order, D)
    temporal_in = normalize(after_spatial).reshape(FRAMES, FRAME_TOK, D) * (1.0 + modulation[4]) + modulation[3] + positions[:, None, :]
    temporal_in = temporal_in.astype(jnp.bfloat16).reshape(TOKENS, D)
    framed = (FRAMES, FRAME_TOK, width_win)
    temporal_q = project(temporal_in, temporal_qkv[0]).astype(jnp.bfloat16).reshape(framed)
    temporal_k = project(temporal_in, temporal_qkv[1]).astype(jnp.bfloat16).reshape(framed)
    temporal_v = project(temporal_in, temporal_qkv[2]).astype(jnp.bfloat16).reshape(framed)
    temporal_mixed = temporal_attend(temporal_q, temporal_k, temporal_v).reshape(TOKENS, width_win)
    return after_spatial + modulation[5] * project(temporal_mixed, temporal_out)
```

```python
import functools
import math

import jax
import jax.numpy as jnp
from jax import lax
from jax.experimental import pallas as pl
from jax.experimental.pallas import tpu as pltpu
from jax.sharding import PartitionSpec as P

HEADS = 16
LANES = 128
PACK = 16

epsilon = 1e-06
bf16, f32 = jnp.bfloat16, jnp.float32


def normalize(activations):
    row_mean = jnp.mean(activations, axis=-1, keepdims=True)
    centered = activations - row_mean
    variance = jnp.mean(centered * centered, axis=-1, keepdims=True)
    return centered * lax.rsqrt(variance + epsilon)


def sinusoid_row(position, width):
    half = width // 2
    lane = lax.broadcasted_iota(jnp.int32, (8, width), 1)
    index = jnp.where(lane < half, lane, lane - half).astype(f32)
    angle = position.astype(f32) * jnp.exp(index * (-math.log(10000.0) / half))
    return jnp.where(lane < half, jnp.sin(angle), jnp.cos(angle))


def up_to(count, unit):
    return -(-count // unit) * unit


def pair_window(pair, head_dim, width):
    first = 2 * head_dim * pair
    return first // LANES * LANES, min(up_to(first + 2 * head_dim, LANES), width)


def outer(a, b):
    return lax.dot_general(a, b, (((1,), (1,)), ((), ())), preferred_element_type=f32)


def pair_scores(queries, keys, pair, head_dim):
    width = queries.shape[0]
    start, stop = pair_window(pair, head_dim, width)
    feature = lax.broadcasted_iota(jnp.int32, (stop - start, LANES), 0) + start
    part = queries[start:stop]
    split = []
    for head in (2 * pair, 2 * pair + 1):
        own = (feature >= head * head_dim) & (feature < (head + 1) * head_dim)
        split.append(part * own.astype(f32).astype(bf16))
    columns = jnp.concatenate(split, axis=1)
    return [jnp.dot(rows[:, start:stop], columns, preferred_element_type=f32) for rows in keys]


def attend(head_dim, queries, keys, values, put):
    width, count = queries.shape
    pairs = width // (2 * head_dim)
    factor = head_dim**-0.5 * math.log2(math.e)
    scores = pair_scores(queries, keys, 0, head_dim)
    for pair in range(pairs):
        later = pair_scores(queries, keys, pair + 1, head_dim) if pair + 1 < pairs else None
        top = functools.reduce(jnp.maximum, [jnp.max(part, axis=0, keepdims=True) for part in scores])
        mixed = None
        for part, value in zip(scores, values):
            weight = jnp.exp2((part - top) * factor).astype(bf16)
            term = jnp.dot(value[pair], weight, preferred_element_type=f32)
            mixed = term if mixed is None else mixed + term
        for side in range(2):
            column = slice(side * count, (side + 1) * count)
            put(
                2 * pair + side,
                mixed[side * head_dim : (side + 1) * head_dim, column],
                top[:, column],
                mixed[2 * head_dim : 2 * head_dim + 1, column],
            )
        scores = later


def block_kernel(
    head_dim, frames, tokens_hbm, stale_hbm, spatial_w_hbm, spatial_o_hbm, temporal_w_hbm, temporal_o_hbm,
    table_ref, mix_ref, timestep_ref, order_ref, out_ref, tokens, spatial_in, k0, kv1, stale, v0, v1, v_stale,
    q, q_in, far_out, far_in, far_stat, stat_in, near, near_stat, spatial_w, spatial_o, temporal_w, temporal_o,
    mod, leaving, arriving, mixed_out, mixed_in, load_sem, kv_send, kv_recv, far_send, far_recv, in_send,
    in_recv, back_send, back_recv,
):
    chunks, _, pixels, _ = leaving.shape
    rows = frames * pixels
    width, feature_width = spatial_o.shape
    heads = width // head_dim
    pairs = heads // 2
    base = width // LANES * LANES
    factor = head_dim**-0.5 * math.log2(math.e)
    device = lax.axis_index("patch")
    slot, quarter = device // 4, device % 4

    def flip(value, mask):
        bit = value // mask % 2
        return value + mask - 2 * mask * bit

    def peer(step):
        other = slot
        mask = 1
        while mask <= step:
            if step & mask:
                other = flip(other, mask)
            mask *= 2
        return other, other * 4 + quarter

    across, beside_me = flip(device, 2), flip(device, 1)

    def load(at, source, target):
        return pltpu.make_async_copy(source, target, load_sem.at[at])

    part_of = lambda ref, part: ref.at[pl.ds(part * width, width)]
    loads = [load(0, tokens_hbm, tokens)]
    loads += [load(1 + part, part_of(spatial_w_hbm, part), part_of(spatial_w, part)) for part in range(3)]
    loads += [
        load(4, stale_hbm, stale),
        load(5, spatial_o_hbm, spatial_o),
        load(6, temporal_w_hbm, temporal_w),
        load(7, temporal_o_hbm, temporal_o),
    ]
    loads[0].start()
    loads[1].start()

    barrier = pltpu.get_barrier_semaphore()
    others = [across, beside_me] + [peer(step)[1] for step in range(1, frames)]
    for other in others:
        pl.semaphore_signal(
            barrier, inc=1, device_id={"patch": other}, device_id_type=pl.DeviceIdType.MESH
        )

    emb = sinusoid_row(timestep_ref[0], feature_width)
    mod[0:6] = table_ref[...] + mix_ref[...] * emb[0:6]
    mod[6:7] = sinusoid_row(order_ref[slot], feature_width)[0:1]
    pl.semaphore_wait(barrier, len(others))

    def remote(source, target, send, recv, other):
        return pltpu.make_async_remote_copy(
            src_ref=source, dst_ref=target, send_sem=send, recv_sem=recv,
            device_id={"patch": other}, device_id_type=pl.DeviceIdType.MESH,
        )

    beside = remote(stale_hbm, kv1, kv_send.at[0], kv_recv.at[0], beside_me)

    def ask(c):
        return remote(q.at[c], q_in.at[c], far_send.at[0, c], far_recv.at[0, c], across)

    def answers(c):
        return (
            remote(far_out.at[c], far_in.at[c], far_send.at[1, c], far_recv.at[1, c], across),
            remote(far_stat.at[c], stat_in.at[c], far_send.at[2, c], far_recv.at[2, c], across),
        )

    loads[0].wait()
    beside.start()
    for one in loads[2:]:
        one.start()
    loads[1].wait()

    group = spatial_in.shape[1]
    per_group = group // rows

    def queries(g, carry):
        wide = tokens[g].astype(f32)
        x = (normalize(wide) * (1.0 + mod[1:2]) + mod[0:1]).astype(bf16)
        spatial_in[g] = x
        fresh = outer(spatial_w[:width], x).astype(bf16)
        for i in range(per_group):
            q[g * per_group + i] = fresh[:, i * rows : (i + 1) * rows]

        @pl.when(g == 0)
        def _():
            for c in range(min(2, chunks)):
                ask(c).start()

        return carry

    ahead = min(2, chunks)
    lax.fori_loop(0, spatial_in.shape[0], queries, 0)
    loads[2].wait()
    loads[3].wait()
    tail = (lax.broadcasted_iota(jnp.int32, (PACK, group), 0) == 0).astype(f32).astype(bf16)

    def keys_values(g, carry):
        x = spatial_in[g]
        here = pl.ds(pl.multiple_of(g * group, group), group)
        k0[here, :] = outer(x, spatial_w[width : 2 * width]).astype(bf16)
        fresh = outer(spatial_w[2 * width :], x).astype(bf16)
        for pair in range(pairs):
            v0[pair, : 2 * head_dim, here] = fresh[2 * head_dim * pair : 2 * head_dim * (pair + 1)]
            for ref in (v0, v1, v_stale):
                ref[pair, 2 * head_dim :, here] = tail
        return carry

    lax.fori_loop(0, spatial_in.shape[0], keys_values, 0)

    def turn(source, target):
        def body(g, carry):
            here = pl.ds(pl.multiple_of(g * group, group), group)
            turned = source[here, base:].T
            for pair in range(pairs):
                at = width - base + 2 * head_dim * pair
                target[pair, : 2 * head_dim, here] = turned[at : at + 2 * head_dim]
            return carry

        lax.fori_loop(0, spatial_in.shape[0], body, 0)

    for one in loads[4:]:
        one.wait()
    turn(stale, v_stale)
    beside.wait_recv()
    turn(kv1, v1)

    def serve(c):
        def put(head, mixed, top, total):
            far_out[c, head * head_dim : (head + 1) * head_dim] = mixed.astype(bf16)
            far_stat[c, head : head + 1] = top
            far_stat[c, heads + head : heads + head + 1] = total

        ask(c).wait_recv()
        attend(head_dim, q_in[c], (stale, kv1), (v_stale, v1), put)
        for one in answers(c):
            one.start()

        @pl.when(c + ahead < chunks)
        def _():
            ask(c + ahead).start()

    def close(c):
        def put(head, mixed, top, total):
            near[c, head * head_dim : (head + 1) * head_dim] = mixed
            near_stat[c, head : head + 1] = top
            near_stat[c, heads + head : heads + head + 1] = total

        attend(head_dim, q[c], (k0, kv1), (v0, v1), put)

    def inward(c, step):
        other, target = peer(step)
        return remote(
            leaving.at[c, other], arriving.at[c, slot], in_send.at[c, step], in_recv.at[c, step], target
        )

    def backward(c, step):
        other, target = peer(step)
        return remote(
            mixed_out.at[c, other], mixed_in.at[c, slot], back_send.at[c, step], back_recv.at[c, step], target
        )

    def join(c):
        for one in answers(c):
            one.wait_recv()
        near_top, near_sum = near_stat[c, :heads], near_stat[c, heads:]
        far_top, far_sum = stat_in[c, :heads], stat_in[c, heads:]
        best = jnp.maximum(near_top, far_top)
        near_part = jnp.exp2((near_top - best) * factor)
        far_part = jnp.exp2((far_top - best) * factor)
        inverse = 1.0 / (near_sum * near_part + far_sum * far_part)
        near_part, far_part = near_part * inverse, far_part * inverse
        shares = []
        for head in range(heads):
            here = slice(head * head_dim, (head + 1) * head_dim)
            shares.append(
                near[c, here] * near_part[head : head + 1]
                + far_in[c, here].astype(f32) * far_part[head : head + 1]
            )
        mixed = jnp.concatenate(shares, axis=0).T.astype(bf16)
        projected = jnp.dot(mixed, spatial_o[...], preferred_element_type=f32)
        after = tokens[c // per_group, pl.ds(pl.multiple_of(c % per_group * rows, rows), rows)].astype(f32)
        after = after + mod[2:3] * projected
        out_ref[c] = after
        temporal_in = normalize(after) * (1.0 + mod[4:5]) + mod[3:4] + mod[6:7]
        leaving[c] = temporal_in.astype(bf16).reshape(frames, pixels, feature_width)
        for step in range(1, frames):
            inward(c, step).start()
        arriving[c, slot] = leaving[c, slot]

    def temporal(c):
        for step in range(1, frames):
            inward(c, step).wait_recv()
        x = arriving[c].reshape(rows, feature_width)
        turned = (heads, head_dim, rows)
        q_all, k_all, v_all = (
            outer(temporal_w[part * width : (part + 1) * width], x).astype(bf16).astype(f32)
            for part in range(3)
        )
        shift = lambda a, step: pltpu.roll(a, (frames - step) * pixels, 1) if step else a
        scores = [
            jnp.sum((q_all * shift(k_all, step)).reshape(turned), axis=1, keepdims=True) * head_dim**-0.5
            for step in range(frames)
        ]
        top = functools.reduce(jnp.maximum, scores)
        exps = [jnp.exp(part - top) for part in scores]
        inverse = 1.0 / functools.reduce(jnp.add, exps)
        mixed = None
        for step, part in enumerate(exps):
            weight = (part * inverse).astype(bf16).astype(f32)
            term = weight * shift(v_all, step).reshape(turned)
            mixed = term if mixed is None else mixed + term
        mixed = mixed.reshape(width, rows).T.astype(bf16)
        mixed_out[c] = mixed.reshape(frames, pixels, width)
        for step in range(1, frames):
            backward(c, step).start()
        mixed_in[c, slot] = mixed_out[c, slot]

    def stage(k, carry):
        @pl.when(k < chunks)
        def _():
            close(k)
            serve(k)

        @pl.when(k >= 3)
        def _():
            temporal(k - 3)

        @pl.when((k >= 1) & (k <= chunks))
        def _():
            join(k - 1)

        return carry

    def third(c, carry):
        for step in range(1, frames):
            backward(c, step).wait_recv()
        mixed = mixed_in[c].reshape(rows, width)
        projected = jnp.dot(mixed, temporal_o[...], preferred_element_type=f32)
        out_ref[c] = out_ref[c] + mod[5:6] * projected
        return carry

    lax.fori_loop(0, chunks + 3, stage, 0)
    lax.fori_loop(0, chunks, third, 0)

    def drain(c, carry):
        ask(c).wait_send()
        for one in answers(c):
            one.wait_send()
        for step in range(1, frames):
            inward(c, step).wait_send()
            backward(c, step).wait_send()
        return carry

    lax.fori_loop(0, chunks, drain, 0)
    beside.wait_send()


def per_device(
    tokens,
    stale_kv,
    mod_table,
    mod_mix,
    timestep,
    frame_order,
    spatial_qkv,
    spatial_out,
    temporal_qkv,
    temporal_out,
):
    frames = lax.axis_size("patch") // 4
    row_count, feature_width = tokens.shape
    width = spatial_out.shape[0]
    head_dim = feature_width // HEADS
    heads = width // head_dim
    pairs = heads // 2
    rows = LANES
    chunks = row_count // rows
    pixels = rows // frames
    group = min(2 * rows, row_count)
    grouped = (row_count // group, group, feature_width)
    turned = lambda w: jnp.swapaxes(w, 1, 2).reshape(3 * width, feature_width)
    flat = (row_count, feature_width)
    chunked = (chunks, rows, feature_width)
    exchanged = (chunks, frames, pixels)
    value_shape = (pairs, 2 * head_dim + PACK, row_count)
    stat_shape = (chunks, 2 * heads, rows)
    anywhere = pl.BlockSpec(memory_space=pl.ANY)
    vmem = pl.BlockSpec(memory_space=pltpu.VMEM)
    smem = pl.BlockSpec(memory_space=pltpu.SMEM)
    out = pl.pallas_call(
        functools.partial(block_kernel, head_dim, frames),
        in_specs=[anywhere] * 6 + [vmem, vmem, smem, smem],
        out_specs=vmem,
        out_shape=jax.ShapeDtypeStruct(chunked, f32),
        scratch_shapes=[
            pltpu.VMEM(grouped, bf16),
            pltpu.VMEM(grouped, bf16),
            pltpu.VMEM((row_count, width), bf16),
            pltpu.VMEM(flat, bf16),
            pltpu.VMEM(flat, bf16),
            pltpu.VMEM(value_shape, bf16),
            pltpu.VMEM(value_shape, bf16),
            pltpu.VMEM(value_shape, bf16),
            pltpu.VMEM((chunks, width, rows), bf16),
            pltpu.VMEM((chunks, width, rows), bf16),
            pltpu.VMEM((chunks, width, rows), bf16),
            pltpu.VMEM((chunks, width, rows), bf16),
            pltpu.VMEM(stat_shape, f32),
            pltpu.VMEM(stat_shape, f32),
            pltpu.VMEM((chunks, width, rows), f32),
            pltpu.VMEM(stat_shape, f32),
            pltpu.VMEM((3 * width, feature_width), bf16),
            pltpu.VMEM((width, feature_width), bf16),
            pltpu.VMEM((3 * width, feature_width), bf16),
            pltpu.VMEM((width, feature_width), bf16),
            pltpu.VMEM((8, feature_width), f32),
            pltpu.VMEM(exchanged + (feature_width,), bf16),
            pltpu.VMEM(exchanged + (feature_width,), bf16),
            pltpu.VMEM(exchanged + (width,), bf16),
            pltpu.VMEM(exchanged + (width,), bf16),
            pltpu.SemaphoreType.DMA((8,)),
            pltpu.SemaphoreType.DMA((1,)),
            pltpu.SemaphoreType.DMA((1,)),
            pltpu.SemaphoreType.DMA((3, chunks)),
            pltpu.SemaphoreType.DMA((3, chunks)),
            pltpu.SemaphoreType.DMA((chunks, frames)),
            pltpu.SemaphoreType.DMA((chunks, frames)),
            pltpu.SemaphoreType.DMA((chunks, frames)),
            pltpu.SemaphoreType.DMA((chunks, frames)),
        ],
        compiler_params=pltpu.CompilerParams(
            collective_id=0, has_side_effects=True, vmem_limit_bytes=60 * 1024 * 1024
        ),
        name="denoising_block",
    )(
        tokens.reshape(grouped), stale_kv, turned(spatial_qkv), spatial_out,
        turned(temporal_qkv), temporal_out, mod_table, mod_mix, timestep, frame_order,
    )
    return out.reshape(flat)


def solution(mesh):
    return jax.shard_map(
        per_device,
        mesh=mesh,
        in_specs=(
            P(("groups", "patch"), None),
            P(("groups", "patch"), None),
            P(),
            P(),
            P("groups"),
            P("groups"),
            P(),
            P(),
            P(),
            P(),
        ),
        out_specs=P(("groups", "patch"), None),
        check_vma=False,
    )
```

```python
import functools
import math

import jax
import jax.numpy as jnp
from jax import lax
from jax.experimental import pallas as pl
from jax.experimental.pallas import tpu as pltpu
from jax.sharding import PartitionSpec as P

HEADS = 16
LANES = 128
PACK = 16

epsilon = 1e-06
bf16, f32 = jnp.bfloat16, jnp.float32


def normalize(activations):
    row_mean = jnp.mean(activations, axis=-1, keepdims=True)
    centered = activations - row_mean
    variance = jnp.mean(centered * centered, axis=-1, keepdims=True)
    return centered * lax.rsqrt(variance + epsilon)


def up_to(count, unit):
    return -(-count // unit) * unit


def sinusoids(positions, width):
    half = width // 2
    count = up_to(len(positions), 8)
    row = lax.broadcasted_iota(jnp.int32, (count, width), 0)
    lane = lax.broadcasted_iota(jnp.int32, (count, width), 1)
    where_to = jnp.zeros((count, width), f32)
    for at, position in enumerate(positions):
        where_to = jnp.where(row == at, position.astype(f32), where_to)
    index = jnp.where(lane < half, lane, lane - half).astype(f32)
    angle = where_to * jnp.exp(index * (-math.log(10000.0) / half))
    return jnp.where(lane < half, jnp.sin(angle), jnp.cos(angle))


def pair_window(pair, head_dim, width):
    first = 2 * head_dim * pair
    return first // LANES * LANES, min(up_to(first + 2 * head_dim, LANES), width)


def outer(a, b):
    return lax.dot_general(a, b, (((1,), (1,)), ((), ())), preferred_element_type=f32)


def pair_scores(queries, keys, pair, head_dim):
    width = queries.shape[0]
    start, stop = pair_window(pair, head_dim, width)
    feature = lax.broadcasted_iota(jnp.int32, (stop - start, LANES), 0) + start
    part = queries[start:stop]
    split = []
    for head in (2 * pair, 2 * pair + 1):
        own = (feature >= head * head_dim) & (feature < (head + 1) * head_dim)
        split.append(part * own.astype(f32).astype(bf16))
    columns = jnp.concatenate(split, axis=1)
    return [jnp.dot(rows[:, start:stop], columns, preferred_element_type=f32) for rows in keys]


def attend(head_dim, queries, keys, values, put):
    width, count = queries.shape
    pairs = width // (2 * head_dim)
    factor = head_dim**-0.5 * math.log2(math.e)
    scores = pair_scores(queries, keys, 0, head_dim)
    for pair in range(pairs):
        later = pair_scores(queries, keys, pair + 1, head_dim) if pair + 1 < pairs else None
        top = functools.reduce(jnp.maximum, [jnp.max(part, axis=0, keepdims=True) for part in scores])
        mixed = None
        for part, value in zip(scores, values):
            weight = jnp.exp2((part - top) * factor).astype(bf16)
            term = jnp.dot(value[pair], weight, preferred_element_type=f32)
            mixed = term if mixed is None else mixed + term
        for side in range(2):
            column = slice(side * count, (side + 1) * count)
            put(
                2 * pair + side,
                mixed[side * head_dim : (side + 1) * head_dim, column],
                top[:, column],
                mixed[2 * head_dim : 2 * head_dim + 1, column],
            )
        scores = later


def block_kernel(
    head_dim, frames, tokens_hbm, stale_hbm, spatial_w_hbm, spatial_o_hbm, temporal_w_hbm, temporal_o_hbm,
    table_hbm, mix_hbm, order_hbm, timestep, out_ref, table, mix, order, tokens, spatial_in, k0, kv1, stale, v0, v1, v_stale,
    q, q_in, far_out, far_in, far_stat, stat_in, near, near_stat, spatial_w, spatial_o, temporal_w, temporal_o,
    mod, place, leaving, arriving, ahead_in, part_out, part_in, mixed_out, mixed_in, load_sem, kv_send, kv_recv,
    far_send, far_recv, ahead_send, ahead_recv, in_send, in_recv, back_send, back_recv,
):
    chunks, _, pixels, _ = leaving.shape
    rows = frames * pixels
    width, feature_width = spatial_o.shape
    heads = width // head_dim
    pairs = heads // 2
    base = width // LANES * LANES
    factor = head_dim**-0.5 * math.log2(math.e)
    device = lax.axis_index("patch")
    slot, quarter = device // 4, device % 4

    def flip(value, mask):
        bit = value // mask % 2
        return value + mask - 2 * mask * bit

    def peer(step):
        other = slot
        mask = 1
        while mask <= step:
            if step & mask:
                other = flip(other, mask)
            mask *= 2
        return other, other * 4 + quarter

    across, beside_me = flip(device, 2), flip(device, 1)

    def load(at, source, target):
        return pltpu.make_async_copy(source, target, load_sem.at[at])

    part_of = lambda ref, part: ref.at[pl.ds(part * width, width)]
    loads = [load(0, tokens_hbm, tokens)]
    loads += [load(1 + part, part_of(spatial_w_hbm, part), part_of(spatial_w, part)) for part in range(3)]
    loads += [
        load(4, stale_hbm, stale),
        load(5, spatial_o_hbm, spatial_o),
        load(6, temporal_w_hbm, temporal_w),
        load(7, temporal_o_hbm, temporal_o),
    ]
    small = [
        load(8, order_hbm, order),
        load(9, table_hbm, table),
        load(10, mix_hbm, mix),
    ]
    for one in small + loads[:2]:
        one.start()

    barrier = pltpu.get_barrier_semaphore()
    others = [across, beside_me] + [peer(step)[1] for step in range(1, frames)]
    for other in others:
        pl.semaphore_signal(
            barrier, inc=1, device_id={"patch": other}, device_id_type=pl.DeviceIdType.MESH
        )

    for one in small:
        one.wait()
    waves = sinusoids([timestep[0]] + [order[f] for f in range(frames)], feature_width)
    place[...] = waves
    mod[0:6] = table[...] + mix[...] * waves[0:1]
    pl.semaphore_wait(barrier, len(others))

    def remote(source, target, send, recv, other):
        return pltpu.make_async_remote_copy(
            src_ref=source, dst_ref=target, send_sem=send, recv_sem=recv,
            device_id={"patch": other}, device_id_type=pl.DeviceIdType.MESH,
        )

    beside = remote(stale_hbm, kv1, kv_send.at[0], kv_recv.at[0], beside_me)

    def ask(c):
        return remote(q.at[c], q_in.at[c], far_send.at[0, c], far_recv.at[0, c], across)

    def answers(c):
        return (
            remote(far_out.at[c], far_in.at[c], far_send.at[1, c], far_recv.at[1, c], across),
            remote(far_stat.at[c], stat_in.at[c], far_send.at[2, c], far_recv.at[2, c], across),
        )

    group = spatial_in.shape[1]
    per_group = group // rows
    early = ahead_in.shape[0]
    lead = min(2, chunks)
    plain = chunks - early

    def send_ahead(c, step):
        other, target = peer(step)
        at = pl.multiple_of(c % per_group * rows + other * pixels, pixels)
        return remote(
            tokens_hbm.at[c // per_group, pl.ds(at, pixels)], ahead_in.at[c - plain, slot],
            ahead_send.at[c - plain, step], ahead_recv.at[c - plain, step], target,
        )

    for c in range(plain, chunks):
        for step in range(1, frames):
            send_ahead(c, step).start()
    loads[0].wait()
    beside.start()
    for one in loads[2:]:
        one.start()
    loads[1].wait()

    def queries(g, carry):
        wide = tokens[g].astype(f32)
        x = (normalize(wide) * (1.0 + mod[1:2]) + mod[0:1]).astype(bf16)
        spatial_in[g] = x
        fresh = outer(spatial_w[:width], x).astype(bf16)
        for i in range(per_group):
            q[g * per_group + i] = fresh[:, i * rows : (i + 1) * rows]

        @pl.when(g == 0)
        def _():
            for c in range(lead):
                ask(c).start()

        return carry

    lax.fori_loop(0, spatial_in.shape[0], queries, 0)
    loads[2].wait()
    loads[3].wait()
    tail = (lax.broadcasted_iota(jnp.int32, (PACK, group), 0) == 0).astype(f32).astype(bf16)

    def keys_values(g, carry):
        x = spatial_in[g]
        here = pl.ds(pl.multiple_of(g * group, group), group)
        k0[here, :] = outer(x, spatial_w[width : 2 * width]).astype(bf16)
        fresh = outer(spatial_w[2 * width :], x).astype(bf16)
        for pair in range(pairs):
            v0[pair, : 2 * head_dim, here] = fresh[2 * head_dim * pair : 2 * head_dim * (pair + 1)]
            for ref in (v0, v1, v_stale):
                ref[pair, 2 * head_dim :, here] = tail
        return carry

    lax.fori_loop(0, spatial_in.shape[0], keys_values, 0)

    def turn(source, target):
        def body(g, carry):
            here = pl.ds(pl.multiple_of(g * group, group), group)
            turned = source[here, base:].T
            for pair in range(pairs):
                at = width - base + 2 * head_dim * pair
                target[pair, : 2 * head_dim, here] = turned[at : at + 2 * head_dim]
            return carry

        lax.fori_loop(0, spatial_in.shape[0], body, 0)

    for one in loads[4:]:
        one.wait()
    turn(stale, v_stale)
    beside.wait_recv()
    turn(kv1, v1)

    def serve(c):
        def put(head, mixed, top, total):
            far_out[c, head * head_dim : (head + 1) * head_dim] = mixed.astype(bf16)
            far_stat[c, head : head + 1] = top
            far_stat[c, heads + head : heads + head + 1] = total

        ask(c).wait_recv()
        attend(head_dim, q_in[c], (stale, kv1), (v_stale, v1), put)
        for one in answers(c):
            one.start()

        @pl.when(c + lead < chunks)
        def _():
            ask(c + lead).start()

    def close(c):
        def put(head, mixed, top, total):
            near[c, head * head_dim : (head + 1) * head_dim] = mixed
            near_stat[c, head : head + 1] = top
            near_stat[c, heads + head : heads + head + 1] = total

        attend(head_dim, q[c], (k0, kv1), (v0, v1), put)

    def inward(c, step):
        other, target = peer(step)
        return remote(
            leaving.at[c, other], arriving.at[c, slot], in_send.at[c, step], in_recv.at[c, step], target
        )

    def inward_part(c, step):
        other, target = peer(step)
        return remote(
            part_out.at[c - plain, other], part_in.at[c - plain, slot], in_send.at[c, step],
            in_recv.at[c, step], target,
        )

    def rows_of(c):
        here = pl.ds(pl.multiple_of(c % per_group * rows, rows), rows)
        return tokens[c // per_group, here].astype(f32)

    def to_temporal(after, position):
        return (normalize(after) * (1.0 + mod[4:5]) + mod[3:4] + position).astype(bf16)

    def backward(c, step):
        other, target = peer(step)
        return remote(
            mixed_out.at[c, other], mixed_in.at[c, slot], back_send.at[c, step], back_recv.at[c, step], target
        )

    def join(c):
        for one in answers(c):
            one.wait_recv()
        near_top, near_sum = near_stat[c, :heads], near_stat[c, heads:]
        far_top, far_sum = stat_in[c, :heads], stat_in[c, heads:]
        best = jnp.maximum(near_top, far_top)
        near_part = jnp.exp2((near_top - best) * factor)
        far_part = jnp.exp2((far_top - best) * factor)
        inverse = 1.0 / (near_sum * near_part + far_sum * far_part)
        near_part, far_part = near_part * inverse, far_part * inverse
        shares = []
        for head in range(heads):
            here = slice(head * head_dim, (head + 1) * head_dim)
            shares.append(
                near[c, here] * near_part[head : head + 1]
                + far_in[c, here].astype(f32) * far_part[head : head + 1]
            )
        mixed = jnp.concatenate(shares, axis=0).T.astype(bf16)

        @pl.when(c >= plain)
        def _():
            part_out[c - plain] = mixed.reshape(frames, pixels, width)
            for step in range(1, frames):
                inward_part(c, step).start()
            part_in[c - plain, slot] = part_out[c - plain, slot]

        projected = jnp.dot(mixed, spatial_o[...], preferred_element_type=f32)
        after = rows_of(c) + mod[2:3] * projected
        out_ref[c] = after

        @pl.when(c < plain)
        def _():
            temporal_in = to_temporal(out_ref[c], place[pl.ds(1 + slot, 1)])
            leaving[c] = temporal_in.reshape(frames, pixels, feature_width)
            for step in range(1, frames):
                inward(c, step).start()
            arriving[c, slot] = leaving[c, slot]

        @pl.when(c >= plain)
        def _():
            here = pl.ds(pl.multiple_of(c % per_group * rows + slot * pixels, pixels), pixels)
            ahead_in[c - plain, slot] = tokens[c // per_group, here]

    def complete(c):
        for step in range(1, frames):
            send_ahead(c, step).wait_recv()
            inward_part(c, step).wait_recv()
        part = part_in[c - plain].reshape(rows, width)
        projected = jnp.dot(part, spatial_o[...], preferred_element_type=f32)
        after = ahead_in[c - plain].reshape(rows, feature_width).astype(f32) + mod[2:3] * projected
        position = place[1 : 1 + frames].reshape(frames, 1, feature_width)
        position = jnp.broadcast_to(position, (frames, pixels, feature_width))
        filled = to_temporal(after, position.reshape(rows, feature_width))
        arriving[c] = filled.reshape(frames, pixels, feature_width)

    def temporal(c):
        @pl.when(c < plain)
        def _():
            for step in range(1, frames):
                inward(c, step).wait_recv()

        @pl.when(c >= plain)
        def _():
            complete(c)

        x = arriving[c].reshape(rows, feature_width)
        turned = (heads, head_dim, rows)
        q_all, k_all, v_all = (
            outer(temporal_w[part * width : (part + 1) * width], x).astype(bf16).astype(f32)
            for part in range(3)
        )
        shift = lambda a, step: pltpu.roll(a, (frames - step) * pixels, 1) if step else a
        scores = [
            jnp.sum((q_all * shift(k_all, step)).reshape(turned), axis=1, keepdims=True) * head_dim**-0.5
            for step in range(frames)
        ]
        top = functools.reduce(jnp.maximum, scores)
        exps = [jnp.exp(part - top) for part in scores]
        inverse = 1.0 / functools.reduce(jnp.add, exps)
        mixed = None
        for step, part in enumerate(exps):
            weight = (part * inverse).astype(bf16).astype(f32)
            term = weight * shift(v_all, step).reshape(turned)
            mixed = term if mixed is None else mixed + term
        mixed = mixed.reshape(width, rows).T.astype(bf16)
        mixed_out[c] = mixed.reshape(frames, pixels, width)
        for step in range(1, frames):
            backward(c, step).start()
        mixed_in[c, slot] = mixed_out[c, slot]

    def stage(k, carry):
        @pl.when(k < chunks)
        def _():
            close(k)
            serve(k)

        @pl.when(k >= 3)
        def _():
            temporal(k - 3)

        @pl.when((k >= 1) & (k <= chunks))
        def _():
            join(k - 1)

        return carry

    def third(c, carry):
        for step in range(1, frames):
            backward(c, step).wait_recv()
        mixed = mixed_in[c].reshape(rows, width)
        projected = jnp.dot(mixed, temporal_o[...], preferred_element_type=f32)
        out_ref[c] = out_ref[c] + mod[5:6] * projected
        return carry

    lax.fori_loop(0, chunks + 3, stage, 0)
    lax.fori_loop(0, chunks, third, 0)

    def drain(c, carry):
        ask(c).wait_send()
        for one in answers(c):
            one.wait_send()
        for step in range(1, frames):
            backward(c, step).wait_send()

        @pl.when(c < plain)
        def _():
            for step in range(1, frames):
                inward(c, step).wait_send()

        @pl.when(c >= plain)
        def _():
            for step in range(1, frames):
                inward_part(c, step).wait_send()
                send_ahead(c, step).wait_send()

        return carry

    lax.fori_loop(0, chunks, drain, 0)
    beside.wait_send()


def per_device(
    tokens,
    stale_kv,
    mod_table,
    mod_mix,
    timestep,
    frame_order,
    spatial_qkv,
    spatial_out,
    temporal_qkv,
    temporal_out,
):
    frames = lax.axis_size("patch") // 4
    row_count, feature_width = tokens.shape
    width = spatial_out.shape[0]
    head_dim = feature_width // HEADS
    heads = width // head_dim
    pairs = heads // 2
    rows = LANES
    chunks = row_count // rows
    pixels = rows // frames
    group = min(2 * rows, row_count)
    grouped = (row_count // group, group, feature_width)
    turned = lambda w: jnp.swapaxes(w, 1, 2).reshape(3 * width, feature_width)
    flat = (row_count, feature_width)
    chunked = (chunks, rows, feature_width)
    exchanged = (chunks, frames, pixels)
    value_shape = (pairs, 2 * head_dim + PACK, row_count)
    stat_shape = (chunks, 2 * heads, rows)
    anywhere = pl.BlockSpec(memory_space=pl.ANY)
    early = min(2, chunks - 1)
    out = pl.pallas_call(
        functools.partial(block_kernel, head_dim, frames),
        in_specs=[anywhere] * 9 + [pl.BlockSpec(memory_space=pltpu.SMEM)],
        out_specs=pl.BlockSpec(memory_space=pltpu.VMEM),
        out_shape=jax.ShapeDtypeStruct(chunked, f32),
        scratch_shapes=[
            pltpu.VMEM(mod_table.shape, f32),
            pltpu.VMEM(mod_mix.shape, f32),
            pltpu.SMEM(frame_order.shape, jnp.int32),
            pltpu.VMEM(grouped, bf16),
            pltpu.VMEM(grouped, bf16),
            pltpu.VMEM((row_count, width), bf16),
            pltpu.VMEM(flat, bf16),
            pltpu.VMEM(flat, bf16),
            pltpu.VMEM(value_shape, bf16),
            pltpu.VMEM(value_shape, bf16),
            pltpu.VMEM(value_shape, bf16),
            pltpu.VMEM((chunks, width, rows), bf16),
            pltpu.VMEM((chunks, width, rows), bf16),
            pltpu.VMEM((chunks, width, rows), bf16),
            pltpu.VMEM((chunks, width, rows), bf16),
            pltpu.VMEM(stat_shape, f32),
            pltpu.VMEM(stat_shape, f32),
            pltpu.VMEM((chunks, width, rows), f32),
            pltpu.VMEM(stat_shape, f32),
            pltpu.VMEM((3 * width, feature_width), bf16),
            pltpu.VMEM((width, feature_width), bf16),
            pltpu.VMEM((3 * width, feature_width), bf16),
            pltpu.VMEM((width, feature_width), bf16),
            pltpu.VMEM((8, feature_width), f32),
            pltpu.VMEM((up_to(1 + frames, 8), feature_width), f32),
            pltpu.VMEM(exchanged + (feature_width,), bf16),
            pltpu.VMEM(exchanged + (feature_width,), bf16),
            pltpu.VMEM((early, frames, pixels, feature_width), bf16),
            pltpu.VMEM((early, frames, pixels, width), bf16),
            pltpu.VMEM((early, frames, pixels, width), bf16),
            pltpu.VMEM(exchanged + (width,), bf16),
            pltpu.VMEM(exchanged + (width,), bf16),
            pltpu.SemaphoreType.DMA((11,)),
            pltpu.SemaphoreType.DMA((1,)),
            pltpu.SemaphoreType.DMA((1,)),
            pltpu.SemaphoreType.DMA((3, chunks)),
            pltpu.SemaphoreType.DMA((3, chunks)),
            pltpu.SemaphoreType.DMA((early, frames)),
            pltpu.SemaphoreType.DMA((early, frames)),
            pltpu.SemaphoreType.DMA((chunks, frames)),
            pltpu.SemaphoreType.DMA((chunks, frames)),
            pltpu.SemaphoreType.DMA((chunks, frames)),
            pltpu.SemaphoreType.DMA((chunks, frames)),
        ],
        compiler_params=pltpu.CompilerParams(
            collective_id=0, has_side_effects=True, vmem_limit_bytes=44 * 1024 * 1024
        ),
        name="denoising_block",
    )(
        *(
            pltpu.with_memory_space_constraint(operand, pltpu.HBM)
            for operand in (
                tokens.reshape(grouped), stale_kv, turned(spatial_qkv), spatial_out, turned(temporal_qkv),
                temporal_out, mod_table, mod_mix, frame_order,
            )
        ),
        timestep,
    )
    return out.reshape(flat)


def solution(mesh):
    return jax.shard_map(
        per_device,
        mesh=mesh,
        in_specs=(
            P(("groups", "patch"), None),
            P(("groups", "patch"), None),
            P(),
            P(),
            P("groups"),
            P("groups"),
            P(),
            P(),
            P(),
            P(),
        ),
        out_specs=P(("groups", "patch"), None),
        check_vma=False,
    )
```

```python
import functools
import math

import jax
import jax.numpy as jnp
from jax import lax
from jax.experimental import pallas as pl
from jax.experimental.pallas import tpu as pltpu
from jax.sharding import PartitionSpec as P

HEADS = 16
LANES = 128
PACK = 16

epsilon = 1e-06
bf16, f32 = jnp.bfloat16, jnp.float32


def normalize(activations):
    row_mean = jnp.mean(activations, axis=-1, keepdims=True)
    centered = activations - row_mean
    variance = jnp.mean(centered * centered, axis=-1, keepdims=True)
    return centered * lax.rsqrt(variance + epsilon)


def up_to(count, unit):
    return -(-count // unit) * unit


def sinusoids(positions, width):
    half = width // 2
    count = up_to(len(positions), 8)
    row = lax.broadcasted_iota(jnp.int32, (count, width), 0)
    lane = lax.broadcasted_iota(jnp.int32, (count, width), 1)
    where_to = jnp.zeros((count, width), f32)
    for at, position in enumerate(positions):
        where_to = jnp.where(row == at, position.astype(f32), where_to)
    index = jnp.where(lane < half, lane, lane - half).astype(f32)
    angle = where_to * jnp.exp(index * (-math.log(10000.0) / half))
    return jnp.where(lane < half, jnp.sin(angle), jnp.cos(angle))


def pair_window(pair, head_dim, width):
    first = 2 * head_dim * pair
    return first // LANES * LANES, min(up_to(first + 2 * head_dim, LANES), width)


def fold(mixed, frames, parts):
    rows, width = mixed.shape
    each = rows // frames // parts
    split = mixed.reshape(frames, parts, each, width)
    side = [split[:, part].reshape(frames * each, width) for part in range(parts)]
    return jnp.concatenate(side, axis=1).reshape(frames, each, parts * width)


def unfold(folded, parts):
    frames, each, wide = folded.shape
    width = wide // parts
    flat = folded.reshape(frames * each, wide)
    side = [flat[:, part * width : (part + 1) * width].reshape(frames, 1, each, width) for part in range(parts)]
    return jnp.concatenate(side, axis=1).reshape(frames * parts * each, width)


def outer(a, b):
    return lax.dot_general(a, b, (((1,), (1,)), ((), ())), preferred_element_type=f32)


def pair_scores(queries, keys, pair, head_dim):
    width = queries.shape[0]
    start, stop = pair_window(pair, head_dim, width)
    feature = lax.broadcasted_iota(jnp.int32, (stop - start, LANES), 0) + start
    part = queries[start:stop]
    split = []
    for head in (2 * pair, 2 * pair + 1):
        own = (feature >= head * head_dim) & (feature < (head + 1) * head_dim)
        split.append(part * own.astype(f32).astype(bf16))
    columns = jnp.concatenate(split, axis=1)
    return [jnp.dot(rows[:, start:stop], columns, preferred_element_type=f32) for rows in keys]


def attend(head_dim, queries, keys, values, put):
    width, count = queries.shape
    pairs = width // (2 * head_dim)
    factor = head_dim**-0.5 * math.log2(math.e)
    scores = pair_scores(queries, keys, 0, head_dim)
    for pair in range(pairs):
        later = pair_scores(queries, keys, pair + 1, head_dim) if pair + 1 < pairs else None
        top = functools.reduce(jnp.maximum, [jnp.max(part, axis=0, keepdims=True) for part in scores])
        mixed = None
        for part, value in zip(scores, values):
            weight = jnp.exp2((part - top) * factor).astype(bf16)
            term = jnp.dot(value[pair], weight, preferred_element_type=f32)
            mixed = term if mixed is None else mixed + term
        for side in range(2):
            column = slice(side * count, (side + 1) * count)
            put(
                2 * pair + side,
                mixed[side * head_dim : (side + 1) * head_dim, column],
                top[:, column],
                mixed[2 * head_dim : 2 * head_dim + 1, column],
            )
        scores = later


def block_kernel(
    head_dim, frames, tokens_hbm, stale_hbm, spatial_w_hbm, spatial_o_hbm, temporal_w_hbm, temporal_o_hbm,
    table_hbm, mix_hbm, order_hbm, timestep, out_ref, table, mix, order, tokens, spatial_in, k0, kv1, stale, v0, v1, v_stale,
    q, q_in, far_out, far_in, far_stat, stat_in, near, near_stat, spatial_w, spatial_o, temporal_w, temporal_o,
    mod, place, leaving, arriving, ahead_in, part_out, part_in, mixed_out, mixed_in, load_sem, kv_send, kv_recv,
    far_send, far_recv, ahead_send, ahead_recv, in_send, in_recv, back_send, back_recv,
):
    chunks, _, pixels, _ = leaving.shape
    rows = frames * pixels
    width, feature_width = spatial_o.shape
    heads = width // head_dim
    pairs = heads // 2
    parts = mixed_in.shape[3] // width
    base = width // LANES * LANES
    factor = head_dim**-0.5 * math.log2(math.e)
    device = lax.axis_index("patch")
    slot, quarter = device // 4, device % 4

    def flip(value, mask):
        bit = value // mask % 2
        return value + mask - 2 * mask * bit

    def peer(step):
        other = slot
        mask = 1
        while mask <= step:
            if step & mask:
                other = flip(other, mask)
            mask *= 2
        return other, other * 4 + quarter

    across, beside_me = flip(device, 2), flip(device, 1)

    def load(at, source, target):
        return pltpu.make_async_copy(source, target, load_sem.at[at])

    part_of = lambda ref, part: ref.at[pl.ds(part * width, width)]
    loads = [load(0, tokens_hbm.at[0], tokens.at[0])]
    loads += [load(1 + part, part_of(spatial_w_hbm, part), part_of(spatial_w, part)) for part in range(3)]
    loads += [
        load(4, stale_hbm, stale),
        load(5, spatial_o_hbm, spatial_o),
        load(6, temporal_w_hbm, temporal_w),
        load(7, temporal_o_hbm, temporal_o),
    ]
    rest = [load(11 + g, tokens_hbm.at[g], tokens.at[g]) for g in range(1, tokens.shape[0])]
    small = [
        load(8, order_hbm, order),
        load(9, table_hbm, table),
        load(10, mix_hbm, mix),
    ]
    for one in small + loads[:2] + rest:
        one.start()

    barrier = pltpu.get_barrier_semaphore()
    others = [across, beside_me] + [peer(step)[1] for step in range(1, frames)]
    for other in others:
        pl.semaphore_signal(
            barrier, inc=1, device_id={"patch": other}, device_id_type=pl.DeviceIdType.MESH
        )

    pl.semaphore_wait(barrier, len(others))

    def remote(source, target, send, recv, other):
        return pltpu.make_async_remote_copy(
            src_ref=source, dst_ref=target, send_sem=send, recv_sem=recv,
            device_id={"patch": other}, device_id_type=pl.DeviceIdType.MESH,
        )

    beside = remote(stale_hbm, kv1, kv_send.at[0], kv_recv.at[0], beside_me)

    def ask(c):
        return remote(q.at[c], q_in.at[c], far_send.at[0, c], far_recv.at[0, c], across)

    def answers(c):
        return (
            remote(far_out.at[c], far_in.at[c], far_send.at[1, c], far_recv.at[1, c], across),
            remote(far_stat.at[c], stat_in.at[c], far_send.at[2, c], far_recv.at[2, c], across),
        )

    group = spatial_in.shape[1]
    per_group = group // rows
    early = ahead_in.shape[0]
    lead = min(2, chunks)
    plain = chunks - early

    def send_ahead(c, step):
        other, target = peer(step)
        at = pl.multiple_of(c % per_group * rows + other * pixels, pixels)
        return remote(
            tokens_hbm.at[c // per_group, pl.ds(at, pixels)], ahead_in.at[c - plain, slot],
            ahead_send.at[c - plain, step], ahead_recv.at[c - plain, step], target,
        )

    for c in range(plain, chunks):
        for step in range(1, frames):
            send_ahead(c, step).start()
    beside.start()
    for one in small:
        one.wait()
    waves = sinusoids([timestep[0]] + [order[f] for f in range(frames)], feature_width)
    place[...] = waves
    mod[0:6] = table[...] + mix[...] * waves[0:1]
    loads[0].wait()
    for one in loads[2:]:
        one.start()
    loads[1].wait()

    def queries(g, at, count):
        x = tokens[g, at : at + count].astype(f32)
        x = (normalize(x) * (1.0 + mod[1:2]) + mod[0:1]).astype(bf16)
        spatial_in[g, at : at + count] = x
        fresh = outer(spatial_w[:width], x).astype(bf16)
        for i in range(count // rows):
            c = g * per_group + at // rows + i
            q[c] = fresh[:, i * rows : (i + 1) * rows]
            if c < lead:
                ask(c).start()

    for at in range(0, group, rows):
        queries(0, at, rows)
    for g, one in enumerate(rest):
        one.wait()
        queries(g + 1, 0, group)
    loads[2].wait()
    loads[3].wait()
    tail = (lax.broadcasted_iota(jnp.int32, (PACK, group), 0) == 0).astype(f32).astype(bf16)

    def keys_values(g, carry):
        x = spatial_in[g]
        here = pl.ds(pl.multiple_of(g * group, group), group)
        k0[here, :] = outer(x, spatial_w[width : 2 * width]).astype(bf16)
        fresh = outer(spatial_w[2 * width :], x).astype(bf16)
        for pair in range(pairs):
            v0[pair, : 2 * head_dim, here] = fresh[2 * head_dim * pair : 2 * head_dim * (pair + 1)]
            for ref in (v0, v1, v_stale):
                ref[pair, 2 * head_dim :, here] = tail
        return carry

    lax.fori_loop(0, spatial_in.shape[0], keys_values, 0)

    def turn(source, target):
        def body(g, carry):
            here = pl.ds(pl.multiple_of(g * group, group), group)
            turned = source[here, base:].T
            for pair in range(pairs):
                at = width - base + 2 * head_dim * pair
                target[pair, : 2 * head_dim, here] = turned[at : at + 2 * head_dim]
            return carry

        lax.fori_loop(0, spatial_in.shape[0], body, 0)

    for one in loads[4:]:
        one.wait()
    turn(stale, v_stale)
    beside.wait_recv()
    turn(kv1, v1)

    def serve(c):
        def put(head, mixed, top, total):
            far_out[c, head * head_dim : (head + 1) * head_dim] = mixed.astype(bf16)
            far_stat[c, head : head + 1] = top
            far_stat[c, heads + head : heads + head + 1] = total

        ask(c).wait_recv()
        attend(head_dim, q_in[c], (stale, kv1), (v_stale, v1), put)
        for one in answers(c):
            one.start()

        @pl.when(c + lead < chunks)
        def _():
            ask(c + lead).start()

    def close(c):
        def put(head, mixed, top, total):
            near[c, head * head_dim : (head + 1) * head_dim] = mixed
            near_stat[c, head : head + 1] = top
            near_stat[c, heads + head : heads + head + 1] = total

        attend(head_dim, q[c], (k0, kv1), (v0, v1), put)

    def inward(c, step):
        other, target = peer(step)
        return remote(
            leaving.at[c, other], arriving.at[c, slot], in_send.at[c, step], in_recv.at[c, step], target
        )

    def inward_part(c, step):
        other, target = peer(step)
        return remote(
            part_out.at[c - plain, other], part_in.at[c - plain, slot], in_send.at[c, step],
            in_recv.at[c, step], target,
        )

    def rows_of(c):
        here = pl.ds(pl.multiple_of(c % per_group * rows, rows), rows)
        return tokens[c // per_group, here].astype(f32)

    def to_temporal(after, position):
        return (normalize(after) * (1.0 + mod[4:5]) + mod[3:4] + position).astype(bf16)

    def backward(c, step):
        other, target = peer(step)
        return remote(
            mixed_out.at[c, other], mixed_in.at[c, slot], back_send.at[c, step], back_recv.at[c, step], target
        )

    def join(c):
        for one in answers(c):
            one.wait_recv()
        near_top, near_sum = near_stat[c, :heads], near_stat[c, heads:]
        far_top, far_sum = stat_in[c, :heads], stat_in[c, heads:]
        best = jnp.maximum(near_top, far_top)
        near_part = jnp.exp2((near_top - best) * factor)
        far_part = jnp.exp2((far_top - best) * factor)
        inverse = 1.0 / (near_sum * near_part + far_sum * far_part)
        near_part, far_part = near_part * inverse, far_part * inverse
        shares = []
        for head in range(heads):
            here = slice(head * head_dim, (head + 1) * head_dim)
            shares.append(
                near[c, here] * near_part[head : head + 1]
                + far_in[c, here].astype(f32) * far_part[head : head + 1]
            )
        mixed = jnp.concatenate(shares, axis=0).T.astype(bf16)

        @pl.when(c >= plain)
        def _():
            part_out[c - plain] = fold(mixed, frames, parts)
            for step in range(1, frames):
                inward_part(c, step).start()
            part_in[c - plain, slot] = part_out[c - plain, slot]

        projected = jnp.dot(mixed, spatial_o[...], preferred_element_type=f32)
        after = rows_of(c) + mod[2:3] * projected
        out_ref[c] = after

        @pl.when(c < plain)
        def _():
            temporal_in = to_temporal(out_ref[c], place[pl.ds(1 + slot, 1)])
            leaving[c] = temporal_in.reshape(frames, pixels, feature_width)
            for step in range(1, frames):
                inward(c, step).start()
            arriving[c, slot] = leaving[c, slot]

        @pl.when(c >= plain)
        def _():
            here = pl.ds(pl.multiple_of(c % per_group * rows + slot * pixels, pixels), pixels)
            ahead_in[c - plain, slot] = tokens[c // per_group, here]

    def complete(c):
        for step in range(1, frames):
            send_ahead(c, step).wait_recv()
            inward_part(c, step).wait_recv()
        part = unfold(part_in[c - plain], parts)
        projected = jnp.dot(part, spatial_o[...], preferred_element_type=f32)
        after = ahead_in[c - plain].reshape(rows, feature_width).astype(f32) + mod[2:3] * projected
        position = place[1 : 1 + frames].reshape(frames, 1, feature_width)
        position = jnp.broadcast_to(position, (frames, pixels, feature_width))
        filled = to_temporal(after, position.reshape(rows, feature_width))
        arriving[c] = filled.reshape(frames, pixels, feature_width)

    def temporal(c):
        @pl.when(c < plain)
        def _():
            for step in range(1, frames):
                inward(c, step).wait_recv()

        @pl.when(c >= plain)
        def _():
            complete(c)

        x = arriving[c].reshape(rows, feature_width)
        turned = (heads, head_dim, rows)
        q_all, k_all, v_all = (
            outer(temporal_w[part * width : (part + 1) * width], x).astype(bf16).astype(f32)
            for part in range(3)
        )
        shift = lambda a, step: pltpu.roll(a, (frames - step) * pixels, 1) if step else a
        scores = [
            jnp.sum((q_all * shift(k_all, step)).reshape(turned), axis=1, keepdims=True) * head_dim**-0.5
            for step in range(frames)
        ]
        top = functools.reduce(jnp.maximum, scores)
        exps = [jnp.exp(part - top) for part in scores]
        inverse = 1.0 / functools.reduce(jnp.add, exps)
        mixed = None
        for step, part in enumerate(exps):
            weight = (part * inverse).astype(bf16).astype(f32)
            term = weight * shift(v_all, step).reshape(turned)
            mixed = term if mixed is None else mixed + term
        mixed = mixed.reshape(width, rows).T.astype(bf16)
        mixed_out[c] = fold(mixed, frames, parts)
        for step in range(1, frames):
            backward(c, step).start()
        mixed_in[c, slot] = mixed_out[c, slot]

    def third(c):
        for step in range(1, frames):
            backward(c, step).wait_recv()
        mixed = unfold(mixed_in[c], parts)
        projected = jnp.dot(mixed, temporal_o[...], preferred_element_type=f32)
        out_ref[c] = out_ref[c] + mod[5:6] * projected

    plan = []
    for k in range(chunks):
        plan.append((serve, k))
        if k < chunks - 1:
            plan.append((close, k))
        if k >= 3:
            plan.append((temporal, k - 3))
        if k >= 1:
            plan.append((join, k - 1))
    plan += [(close, chunks - 1), (join, chunks - 1)]
    plan += [(temporal, c) for c in range(max(0, chunks - 3), chunks)]
    plan += [(third, c) for c in range(chunks)]

    def turn_of(t, carry):
        for work in (serve, close, temporal, join, third):
            turns = [(at, c) for at, (kind, c) in enumerate(plan) if kind is work]
            due = functools.reduce(jnp.logical_or, [t == at for at, _ in turns])
            chunk = functools.reduce(lambda other, turn: jnp.where(t == turn[0], turn[1], other), turns, 0)

            @pl.when(due)
            def _():
                work(chunk)

        return carry

    lax.fori_loop(0, len(plan), turn_of, 0)

    def drain(c, carry):
        ask(c).wait_send()
        for one in answers(c):
            one.wait_send()
        for step in range(1, frames):
            backward(c, step).wait_send()

        @pl.when(c < plain)
        def _():
            for step in range(1, frames):
                inward(c, step).wait_send()

        @pl.when(c >= plain)
        def _():
            for step in range(1, frames):
                inward_part(c, step).wait_send()
                send_ahead(c, step).wait_send()

        return carry

    lax.fori_loop(0, chunks, drain, 0)
    beside.wait_send()


def per_device(
    tokens,
    stale_kv,
    mod_table,
    mod_mix,
    timestep,
    frame_order,
    spatial_qkv,
    spatial_out,
    temporal_qkv,
    temporal_out,
):
    frames = lax.axis_size("patch") // 4
    row_count, feature_width = tokens.shape
    width = spatial_out.shape[0]
    head_dim = feature_width // HEADS
    heads = width // head_dim
    pairs = heads // 2
    rows = LANES
    chunks = row_count // rows
    pixels = rows // frames
    group = min(2 * rows, row_count)
    grouped = (row_count // group, group, feature_width)
    turned = lambda w: jnp.swapaxes(w, 1, 2).reshape(3 * width, feature_width)
    flat = (row_count, feature_width)
    chunked = (chunks, rows, feature_width)
    exchanged = (chunks, frames, pixels)
    parts = 2 if width % LANES and pixels % (2 * PACK) == 0 else 1
    folded = (frames, pixels // parts, parts * width)
    value_shape = (pairs, 2 * head_dim + PACK, row_count)
    stat_shape = (chunks, 2 * heads, rows)
    anywhere = pl.BlockSpec(memory_space=pl.ANY)
    early = min(2, max(1, chunks - 1))
    out = pl.pallas_call(
        functools.partial(block_kernel, head_dim, frames),
        in_specs=[anywhere] * 9 + [pl.BlockSpec(memory_space=pltpu.SMEM)],
        out_specs=pl.BlockSpec(memory_space=pltpu.VMEM),
        out_shape=jax.ShapeDtypeStruct(chunked, f32),
        scratch_shapes=[
            pltpu.VMEM(mod_table.shape, f32),
            pltpu.VMEM(mod_mix.shape, f32),
            pltpu.SMEM(frame_order.shape, jnp.int32),
            pltpu.VMEM(grouped, bf16),
            pltpu.VMEM(grouped, bf16),
            pltpu.VMEM((row_count, width), bf16),
            pltpu.VMEM(flat, bf16),
            pltpu.VMEM(flat, bf16),
            pltpu.VMEM(value_shape, bf16),
            pltpu.VMEM(value_shape, bf16),
            pltpu.VMEM(value_shape, bf16),
            pltpu.VMEM((chunks, width, rows), bf16),
            pltpu.VMEM((chunks, width, rows), bf16),
            pltpu.VMEM((chunks, width, rows), bf16),
            pltpu.VMEM((chunks, width, rows), bf16),
            pltpu.VMEM(stat_shape, f32),
            pltpu.VMEM(stat_shape, f32),
            pltpu.VMEM((chunks, width, rows), f32),
            pltpu.VMEM(stat_shape, f32),
            pltpu.VMEM((3 * width, feature_width), bf16),
            pltpu.VMEM((width, feature_width), bf16),
            pltpu.VMEM((3 * width, feature_width), bf16),
            pltpu.VMEM((width, feature_width), bf16),
            pltpu.VMEM((8, feature_width), f32),
            pltpu.VMEM((up_to(1 + frames, 8), feature_width), f32),
            pltpu.VMEM(exchanged + (feature_width,), bf16),
            pltpu.VMEM(exchanged + (feature_width,), bf16),
            pltpu.VMEM((early, frames, pixels, feature_width), bf16),
            pltpu.VMEM((early,) + folded, bf16),
            pltpu.VMEM((early,) + folded, bf16),
            pltpu.VMEM((chunks,) + folded, bf16),
            pltpu.VMEM((chunks,) + folded, bf16),
            pltpu.SemaphoreType.DMA((11 + row_count // group,)),
            pltpu.SemaphoreType.DMA((1,)),
            pltpu.SemaphoreType.DMA((1,)),
            pltpu.SemaphoreType.DMA((3, chunks)),
            pltpu.SemaphoreType.DMA((3, chunks)),
            pltpu.SemaphoreType.DMA((early, frames)),
            pltpu.SemaphoreType.DMA((early, frames)),
            pltpu.SemaphoreType.DMA((chunks, frames)),
            pltpu.SemaphoreType.DMA((chunks, frames)),
            pltpu.SemaphoreType.DMA((chunks, frames)),
            pltpu.SemaphoreType.DMA((chunks, frames)),
        ],
        compiler_params=pltpu.CompilerParams(
            collective_id=0, has_side_effects=True, vmem_limit_bytes=44 * 1024 * 1024
        ),
        name="denoising_block",
    )(
        *(
            pltpu.with_memory_space_constraint(operand, pltpu.HBM)
            for operand in (
                tokens.reshape(grouped), stale_kv, turned(spatial_qkv), spatial_out, turned(temporal_qkv),
                temporal_out, mod_table, mod_mix, frame_order,
            )
        ),
        timestep,
    )
    return out.reshape(flat)


def solution(mesh):
    return jax.shard_map(
        per_device,
        mesh=mesh,
        in_specs=(
            P(("groups", "patch"), None),
            P(("groups", "patch"), None),
            P(),
            P(),
            P("groups"),
            P("groups"),
            P(),
            P(),
            P(),
            P(),
        ),
        out_specs=P(("groups", "patch"), None),
        check_vma=False,
    )
```

```python
import functools
import math

import jax
import jax.numpy as jnp
from jax import lax
from jax.experimental import pallas as pl
from jax.experimental.pallas import tpu as pltpu
from jax.sharding import PartitionSpec as P

HEADS = 16
LANES = 128
PACK = 16

epsilon = 1e-06
bf16, f32 = jnp.bfloat16, jnp.float32


def normalize(activations):
    row_mean = jnp.mean(activations, axis=-1, keepdims=True)
    centered = activations - row_mean
    variance = jnp.mean(centered * centered, axis=-1, keepdims=True)
    return centered * lax.rsqrt(variance + epsilon)


def up_to(count, unit):
    return -(-count // unit) * unit


def sinusoids(positions, width):
    half = width // 2
    count = up_to(len(positions), 8)
    row = lax.broadcasted_iota(jnp.int32, (count, width), 0)
    lane = lax.broadcasted_iota(jnp.int32, (count, width), 1)
    where_to = jnp.zeros((count, width), f32)
    for at, position in enumerate(positions):
        where_to = jnp.where(row == at, position.astype(f32), where_to)
    index = jnp.where(lane < half, lane, lane - half).astype(f32)
    angle = where_to * jnp.exp(index * (-math.log(10000.0) / half))
    return jnp.where(lane < half, jnp.sin(angle), jnp.cos(angle))


def pair_window(pair, head_dim, width):
    first = 2 * head_dim * pair
    return first // LANES * LANES, min(up_to(first + 2 * head_dim, LANES), width)


def fold(mixed, frames, parts):
    rows, width = mixed.shape
    each = rows // frames // parts
    split = mixed.reshape(frames, parts, each, width)
    side = [split[:, part].reshape(frames * each, width) for part in range(parts)]
    return jnp.concatenate(side, axis=1).reshape(frames, each, parts * width)


def unfold(folded, parts):
    frames, each, wide = folded.shape
    width = wide // parts
    flat = folded.reshape(frames * each, wide)
    side = [flat[:, part * width : (part + 1) * width].reshape(frames, 1, each, width) for part in range(parts)]
    return jnp.concatenate(side, axis=1).reshape(frames * parts * each, width)


def outer(a, b):
    return lax.dot_general(a, b, (((1,), (1,)), ((), ())), preferred_element_type=f32)


def pair_scores(queries, keys, pair, head_dim):
    width = queries.shape[0]
    start, stop = pair_window(pair, head_dim, width)
    feature = lax.broadcasted_iota(jnp.int32, (stop - start, LANES), 0) + start
    part = queries[start:stop]
    split = []
    for head in (2 * pair, 2 * pair + 1):
        own = (feature >= head * head_dim) & (feature < (head + 1) * head_dim)
        split.append(part * own.astype(f32).astype(bf16))
    columns = jnp.concatenate(split, axis=1)
    return [jnp.dot(rows[:, start:stop], columns, preferred_element_type=f32) for rows in keys]


def attend(head_dim, queries, keys, values, put):
    width, count = queries.shape
    pairs = width // (2 * head_dim)
    factor = head_dim**-0.5 * math.log2(math.e)
    scores = pair_scores(queries, keys, 0, head_dim)
    for pair in range(pairs):
        later = pair_scores(queries, keys, pair + 1, head_dim) if pair + 1 < pairs else None
        top = functools.reduce(jnp.maximum, [jnp.max(part, axis=0, keepdims=True) for part in scores])
        mixed = None
        for part, value in zip(scores, values):
            weight = jnp.exp2((part - top) * factor).astype(bf16)
            term = jnp.dot(value[pair], weight, preferred_element_type=f32)
            mixed = term if mixed is None else mixed + term
        for side in range(2):
            column = slice(side * count, (side + 1) * count)
            put(
                2 * pair + side,
                mixed[side * head_dim : (side + 1) * head_dim, column],
                top[:, column],
                mixed[2 * head_dim : 2 * head_dim + 1, column],
            )
        scores = later


def block_kernel(
    head_dim, frames, tokens_hbm, stale_hbm, spatial_w_hbm, spatial_o_hbm, temporal_w_hbm, temporal_o_hbm,
    table_hbm, mix_hbm, order_hbm, timestep, out_ref, table, mix, order, tokens, spatial_in, k0, kv1, stale, v0, v1, v_stale,
    q, q_in, far_out, far_in, far_stat, stat_in, near, near_stat, spatial_w, spatial_o, temporal_w, temporal_o,
    mod, place, leaving, arriving, ahead_in, part_out, part_in, mixed_out, mixed_in, load_sem, kv_send, kv_recv,
    far_send, far_recv, ahead_send, ahead_recv, in_send, in_recv, back_send, back_recv,
):
    chunks, _, pixels, _ = leaving.shape
    rows = frames * pixels
    width, feature_width = spatial_o.shape
    heads = width // head_dim
    pairs = heads // 2
    parts = mixed_in.shape[3] // width
    base = width // LANES * LANES
    factor = head_dim**-0.5 * math.log2(math.e)
    device = lax.axis_index("patch")
    slot, quarter = device // 4, device % 4

    def flip(value, mask):
        bit = value // mask % 2
        return value + mask - 2 * mask * bit

    def peer(step):
        other = slot
        mask = 1
        while mask <= step:
            if step & mask:
                other = flip(other, mask)
            mask *= 2
        return other, other * 4 + quarter

    across, beside_me = flip(device, 2), flip(device, 1)

    def load(at, source, target):
        return pltpu.make_async_copy(source, target, load_sem.at[at])

    part_of = lambda ref, part: ref.at[pl.ds(part * width, width)]
    loads = [load(0, tokens_hbm.at[0], tokens.at[0])]
    loads += [load(1 + part, part_of(spatial_w_hbm, part), part_of(spatial_w, part)) for part in range(3)]
    loads += [
        load(4, stale_hbm, stale),
        load(5, spatial_o_hbm, spatial_o),
        load(6, temporal_w_hbm, temporal_w),
        load(7, temporal_o_hbm, temporal_o),
    ]
    rest = [load(11 + g, tokens_hbm.at[g], tokens.at[g]) for g in range(1, tokens.shape[0])]
    small = [
        load(8, order_hbm, order),
        load(9, table_hbm, table),
        load(10, mix_hbm, mix),
    ]
    for one in small + loads[:2] + rest:
        one.start()

    barrier = pltpu.get_barrier_semaphore()
    others = [across, beside_me] + [peer(step)[1] for step in range(1, frames)]
    for other in others:
        pl.semaphore_signal(
            barrier, inc=1, device_id={"patch": other}, device_id_type=pl.DeviceIdType.MESH
        )


    def remote(source, target, send, recv, other):
        return pltpu.make_async_remote_copy(
            src_ref=source, dst_ref=target, send_sem=send, recv_sem=recv,
            device_id={"patch": other}, device_id_type=pl.DeviceIdType.MESH,
        )

    beside = remote(stale_hbm, kv1, kv_send.at[0], kv_recv.at[0], beside_me)

    def ask(c):
        return remote(q.at[c], q_in.at[c], far_send.at[0, c], far_recv.at[0, c], across)

    def answers(c):
        return (
            remote(far_out.at[c], far_in.at[c], far_send.at[1, c], far_recv.at[1, c], across),
            remote(far_stat.at[c], stat_in.at[c], far_send.at[2, c], far_recv.at[2, c], across),
        )

    group = spatial_in.shape[1]
    per_group = group // rows
    early = ahead_in.shape[0]
    lead = min(2, chunks)
    plain = chunks - early

    def send_ahead(c, step):
        other, target = peer(step)
        at = pl.multiple_of(c % per_group * rows + other * pixels, pixels)
        return remote(
            tokens_hbm.at[c // per_group, pl.ds(at, pixels)], ahead_in.at[c - plain, slot],
            ahead_send.at[c - plain, step], ahead_recv.at[c - plain, step], target,
        )

    def meet():
        pl.semaphore_wait(barrier, len(others))
        for c in range(plain, chunks):
            for step in range(1, frames):
                send_ahead(c, step).start()
        beside.start()

    for one in small:
        one.wait()
    waves = sinusoids([timestep[0]] + [order[f] for f in range(frames)], feature_width)
    place[...] = waves
    mod[0:6] = table[...] + mix[...] * waves[0:1]
    loads[0].wait()
    for one in loads[2:]:
        one.start()
    loads[1].wait()

    def queries(g, at, count):
        x = tokens[g, at : at + count].astype(f32)
        x = (normalize(x) * (1.0 + mod[1:2]) + mod[0:1]).astype(bf16)
        spatial_in[g, at : at + count] = x
        fresh = outer(spatial_w[:width], x).astype(bf16)
        for i in range(count // rows):
            c = g * per_group + at // rows + i
            q[c] = fresh[:, i * rows : (i + 1) * rows]
            if 0 < c < lead:
                ask(c).start()

    queries(0, 0, rows)
    meet()
    ask(0).start()
    for at in range(rows, group, rows):
        queries(0, at, rows)
    for g, one in enumerate(rest):
        one.wait()
        queries(g + 1, 0, group)
    loads[2].wait()
    loads[3].wait()
    tail = (lax.broadcasted_iota(jnp.int32, (PACK, group), 0) == 0).astype(f32).astype(bf16)

    def keys_values(g, carry):
        x = spatial_in[g]
        here = pl.ds(pl.multiple_of(g * group, group), group)
        k0[here, :] = outer(x, spatial_w[width : 2 * width]).astype(bf16)
        fresh = outer(spatial_w[2 * width :], x).astype(bf16)
        for pair in range(pairs):
            v0[pair, : 2 * head_dim, here] = fresh[2 * head_dim * pair : 2 * head_dim * (pair + 1)]
            for ref in (v0, v1, v_stale):
                ref[pair, 2 * head_dim :, here] = tail
        return carry

    lax.fori_loop(0, spatial_in.shape[0], keys_values, 0)

    def turn(source, target):
        def body(g, carry):
            here = pl.ds(pl.multiple_of(g * group, group), group)
            turned = source[here, base:].T
            for pair in range(pairs):
                at = width - base + 2 * head_dim * pair
                target[pair, : 2 * head_dim, here] = turned[at : at + 2 * head_dim]
            return carry

        lax.fori_loop(0, spatial_in.shape[0], body, 0)

    for one in loads[4:]:
        one.wait()
    turn(stale, v_stale)
    beside.wait_recv()
    turn(kv1, v1)

    def serve(c):
        def put(head, mixed, top, total):
            far_out[c, head * head_dim : (head + 1) * head_dim] = mixed.astype(bf16)
            far_stat[c, head : head + 1] = top
            far_stat[c, heads + head : heads + head + 1] = total

        ask(c).wait_recv()
        attend(head_dim, q_in[c], (stale, kv1), (v_stale, v1), put)
        for one in answers(c):
            one.start()

        @pl.when(c + lead < chunks)
        def _():
            ask(c + lead).start()

    def close(c):
        def put(head, mixed, top, total):
            near[c, head * head_dim : (head + 1) * head_dim] = mixed
            near_stat[c, head : head + 1] = top
            near_stat[c, heads + head : heads + head + 1] = total

        attend(head_dim, q[c], (k0, kv1), (v0, v1), put)

    def inward(c, step):
        other, target = peer(step)
        return remote(
            leaving.at[c, other], arriving.at[c, slot], in_send.at[c, step], in_recv.at[c, step], target
        )

    def inward_part(c, step):
        other, target = peer(step)
        return remote(
            part_out.at[c - plain, other], part_in.at[c - plain, slot], in_send.at[c, step],
            in_recv.at[c, step], target,
        )

    def rows_of(c):
        here = pl.ds(pl.multiple_of(c % per_group * rows, rows), rows)
        return tokens[c // per_group, here].astype(f32)

    def to_temporal(after, position):
        return (normalize(after) * (1.0 + mod[4:5]) + mod[3:4] + position).astype(bf16)

    def backward(c, step):
        other, target = peer(step)
        return remote(
            mixed_out.at[c, other], mixed_in.at[c, slot], back_send.at[c, step], back_recv.at[c, step], target
        )

    def join(c):
        for one in answers(c):
            one.wait_recv()
        near_top, near_sum = near_stat[c, :heads], near_stat[c, heads:]
        far_top, far_sum = stat_in[c, :heads], stat_in[c, heads:]
        best = jnp.maximum(near_top, far_top)
        near_part = jnp.exp2((near_top - best) * factor)
        far_part = jnp.exp2((far_top - best) * factor)
        inverse = 1.0 / (near_sum * near_part + far_sum * far_part)
        near_part, far_part = near_part * inverse, far_part * inverse
        shares = []
        for head in range(heads):
            here = slice(head * head_dim, (head + 1) * head_dim)
            shares.append(
                near[c, here] * near_part[head : head + 1]
                + far_in[c, here].astype(f32) * far_part[head : head + 1]
            )
        mixed = jnp.concatenate(shares, axis=0).T.astype(bf16)

        @pl.when(c >= plain)
        def _():
            part_out[c - plain] = fold(mixed, frames, parts)
            for step in range(1, frames):
                inward_part(c, step).start()
            part_in[c - plain, slot] = part_out[c - plain, slot]

        projected = jnp.dot(mixed, spatial_o[...], preferred_element_type=f32)
        after = rows_of(c) + mod[2:3] * projected
        out_ref[c] = after

        @pl.when(c < plain)
        def _():
            temporal_in = to_temporal(out_ref[c], place[pl.ds(1 + slot, 1)])
            leaving[c] = temporal_in.reshape(frames, pixels, feature_width)
            for step in range(1, frames):
                inward(c, step).start()
            arriving[c, slot] = leaving[c, slot]

        @pl.when(c >= plain)
        def _():
            here = pl.ds(pl.multiple_of(c % per_group * rows + slot * pixels, pixels), pixels)
            ahead_in[c - plain, slot] = tokens[c // per_group, here]

    def complete(c):
        for step in range(1, frames):
            send_ahead(c, step).wait_recv()
            inward_part(c, step).wait_recv()
        part = unfold(part_in[c - plain], parts)
        projected = jnp.dot(part, spatial_o[...], preferred_element_type=f32)
        after = ahead_in[c - plain].reshape(rows, feature_width).astype(f32) + mod[2:3] * projected
        position = place[1 : 1 + frames].reshape(frames, 1, feature_width)
        position = jnp.broadcast_to(position, (frames, pixels, feature_width))
        filled = to_temporal(after, position.reshape(rows, feature_width))
        arriving[c] = filled.reshape(frames, pixels, feature_width)

    def temporal(c):
        @pl.when(c < plain)
        def _():
            for step in range(1, frames):
                inward(c, step).wait_recv()

        @pl.when(c >= plain)
        def _():
            complete(c)

        x = arriving[c].reshape(rows, feature_width)
        turned = (heads, head_dim, rows)
        q_all, k_all, v_all = (
            outer(temporal_w[part * width : (part + 1) * width], x).astype(bf16).astype(f32)
            for part in range(3)
        )
        shift = lambda a, step: pltpu.roll(a, (frames - step) * pixels, 1) if step else a
        scores = [
            jnp.sum((q_all * shift(k_all, step)).reshape(turned), axis=1, keepdims=True) * head_dim**-0.5
            for step in range(frames)
        ]
        top = functools.reduce(jnp.maximum, scores)
        exps = [jnp.exp(part - top) for part in scores]
        inverse = 1.0 / functools.reduce(jnp.add, exps)
        mixed = None
        for step, part in enumerate(exps):
            weight = (part * inverse).astype(bf16).astype(f32)
            term = weight * shift(v_all, step).reshape(turned)
            mixed = term if mixed is None else mixed + term
        mixed = mixed.reshape(width, rows).T.astype(bf16)
        mixed_out[c] = fold(mixed, frames, parts)
        for step in range(1, frames):
            backward(c, step).start()
        mixed_in[c, slot] = mixed_out[c, slot]

    def third(c):
        for step in range(1, frames):
            backward(c, step).wait_recv()
        mixed = unfold(mixed_in[c], parts)
        projected = jnp.dot(mixed, temporal_o[...], preferred_element_type=f32)
        out_ref[c] = out_ref[c] + mod[5:6] * projected

    def drain(c):
        ask(c).wait_send()
        for one in answers(c):
            one.wait_send()
        for step in range(1, frames):
            backward(c, step).wait_send()

        @pl.when(c < plain)
        def _():
            for step in range(1, frames):
                inward(c, step).wait_send()

        @pl.when(c >= plain)
        def _():
            for step in range(1, frames):
                inward_part(c, step).wait_send()
                send_ahead(c, step).wait_send()

    plan = []
    for k in range(chunks):
        plan.append((serve, k))
        if k < chunks - 1:
            plan.append((close, k))
        if k >= 3:
            plan.append((temporal, k - 3))
        if k >= 1:
            plan.append((join, k - 1))
    plan += [(close, chunks - 1), (join, chunks - 1)]
    plan += [(temporal, c) for c in range(max(0, chunks - 3), chunks)]
    plan += [(drain, c) for c in range(chunks)]
    plan += [(third, c) for c in range(chunks)]

    def turn_of(t, carry):
        for work in (serve, close, temporal, join, drain, third):
            turns = [(at, c) for at, (kind, c) in enumerate(plan) if kind is work]
            due = functools.reduce(jnp.logical_or, [t == at for at, _ in turns])
            chunk = functools.reduce(lambda other, turn: jnp.where(t == turn[0], turn[1], other), turns, 0)

            @pl.when(due)
            def _():
                work(chunk)

        return carry

    lax.fori_loop(0, len(plan), turn_of, 0)
    beside.wait_send()


def per_device(
    tokens,
    stale_kv,
    mod_table,
    mod_mix,
    timestep,
    frame_order,
    spatial_qkv,
    spatial_out,
    temporal_qkv,
    temporal_out,
):
    frames = lax.axis_size("patch") // 4
    row_count, feature_width = tokens.shape
    width = spatial_out.shape[0]
    head_dim = feature_width // HEADS
    heads = width // head_dim
    pairs = heads // 2
    rows = LANES
    chunks = row_count // rows
    pixels = rows // frames
    group = min(2 * rows, row_count)
    grouped = (row_count // group, group, feature_width)
    turned = lambda w: jnp.swapaxes(w, 1, 2).reshape(3 * width, feature_width)
    flat = (row_count, feature_width)
    chunked = (chunks, rows, feature_width)
    exchanged = (chunks, frames, pixels)
    parts = 2 if width % LANES and pixels % (2 * PACK) == 0 else 1
    folded = (frames, pixels // parts, parts * width)
    value_shape = (pairs, 2 * head_dim + PACK, row_count)
    stat_shape = (chunks, 2 * heads, rows)
    anywhere = pl.BlockSpec(memory_space=pl.ANY)
    early = min(2, max(1, chunks - 1))
    out = pl.pallas_call(
        functools.partial(block_kernel, head_dim, frames),
        in_specs=[anywhere] * 9 + [pl.BlockSpec(memory_space=pltpu.SMEM)],
        out_specs=pl.BlockSpec(memory_space=pltpu.VMEM),
        out_shape=jax.ShapeDtypeStruct(chunked, f32),
        scratch_shapes=[
            pltpu.VMEM(mod_table.shape, f32),
            pltpu.VMEM(mod_mix.shape, f32),
            pltpu.SMEM(frame_order.shape, jnp.int32),
            pltpu.VMEM(grouped, bf16),
            pltpu.VMEM(grouped, bf16),
            pltpu.VMEM((row_count, width), bf16),
            pltpu.VMEM(flat, bf16),
            pltpu.VMEM(flat, bf16),
            pltpu.VMEM(value_shape, bf16),
            pltpu.VMEM(value_shape, bf16),
            pltpu.VMEM(value_shape, bf16),
            pltpu.VMEM((chunks, width, rows), bf16),
            pltpu.VMEM((chunks, width, rows), bf16),
            pltpu.VMEM((chunks, width, rows), bf16),
            pltpu.VMEM((chunks, width, rows), bf16),
            pltpu.VMEM(stat_shape, f32),
            pltpu.VMEM(stat_shape, f32),
            pltpu.VMEM((chunks, width, rows), f32),
            pltpu.VMEM(stat_shape, f32),
            pltpu.VMEM((3 * width, feature_width), bf16),
            pltpu.VMEM((width, feature_width), bf16),
            pltpu.VMEM((3 * width, feature_width), bf16),
            pltpu.VMEM((width, feature_width), bf16),
            pltpu.VMEM((8, feature_width), f32),
            pltpu.VMEM((up_to(1 + frames, 8), feature_width), f32),
            pltpu.VMEM(exchanged + (feature_width,), bf16),
            pltpu.VMEM(exchanged + (feature_width,), bf16),
            pltpu.VMEM((early, frames, pixels, feature_width), bf16),
            pltpu.VMEM((early,) + folded, bf16),
            pltpu.VMEM((early,) + folded, bf16),
            pltpu.VMEM((chunks,) + folded, bf16),
            pltpu.VMEM((chunks,) + folded, bf16),
            pltpu.SemaphoreType.DMA((11 + row_count // group,)),
            pltpu.SemaphoreType.DMA((1,)),
            pltpu.SemaphoreType.DMA((1,)),
            pltpu.SemaphoreType.DMA((3, chunks)),
            pltpu.SemaphoreType.DMA((3, chunks)),
            pltpu.SemaphoreType.DMA((early, frames)),
            pltpu.SemaphoreType.DMA((early, frames)),
            pltpu.SemaphoreType.DMA((chunks, frames)),
            pltpu.SemaphoreType.DMA((chunks, frames)),
            pltpu.SemaphoreType.DMA((chunks, frames)),
            pltpu.SemaphoreType.DMA((chunks, frames)),
        ],
        compiler_params=pltpu.CompilerParams(
            collective_id=0, has_side_effects=True, vmem_limit_bytes=44 * 1024 * 1024
        ),
        name="denoising_block",
    )(
        *(
            pltpu.with_memory_space_constraint(operand, pltpu.HBM)
            for operand in (
                tokens.reshape(grouped), stale_kv, turned(spatial_qkv), spatial_out, turned(temporal_qkv),
                temporal_out, mod_table, mod_mix, frame_order,
            )
        ),
        timestep,
    )
    return out.reshape(flat)


def solution(mesh):
    return jax.shard_map(
        per_device,
        mesh=mesh,
        in_specs=(
            P(("groups", "patch"), None),
            P(("groups", "patch"), None),
            P(),
            P(),
            P("groups"),
            P("groups"),
            P(),
            P(),
            P(),
            P(),
        ),
        out_specs=P(("groups", "patch"), None),
        check_vma=False,
    )
```
